256 devices in a mesh: groups: 4 (over y, x), mp: 64 (over z, core).
Axes of the slice: x: 2, y: 2, z: 32, core: 2. Of those that a mesh axis runs over, the one named last changes fastest.
The devices are a block of a 4x8x32 slice.
Arguments:
- hidden: bfloat16 [2048, 4096], P(('groups', 'mp')), parts along dimension 0, may hold values from -6 to 6
- norm_gain_attn: float32 [4096], replicated, may hold values from 0.5 to 1.5
- w_query: bfloat16 [4096, 4096], P(None, 'mp'), may hold values from -0.09375 to 0.09375
- entering_kv: bfloat16 [32, 2048, 8192], P('groups', 'mp'), parts along dimension 0, may hold values from -60 to 60
- cached_kv: bfloat16 [32, 2048, 8192], P('groups', None, 'mp'), parts along dimension 0, may hold values from -60 to 60
- enc_lengths: int32 [2, 32], P(None, 'groups'), parts along dimension 1, may hold values from 128 to 2048
- w_out: bfloat16 [4096, 4096], P('mp'), may hold values from -0.09375 to 0.09375
- norm_gain_ffn: float32 [4096], replicated, may hold values from 0.5 to 1.5
- w_gate: bfloat16 [4096, 10240], P(None, 'mp'), may hold values from -0.09375 to 0.09375
- w_up: bfloat16 [4096, 10240], P(None, 'mp'), may hold values from -0.09375 to 0.09375
- w_down: bfloat16 [10240, 4096], P('mp'), may hold values from -0.0625 to 0.0625
Outputs:
- output: bfloat16 [2048, 4096], P(('groups', 'mp')), parts along dimension 0
The draws below stay inside these ranges and needn't reach their ends.
There are 4 independent parts, one for each index of `groups`. The reference program is written for one: setup_inputs(seed, part) draws one part's arguments, and reference() takes and returns one part's arrays. A program takes and returns all parts, laid end to end along the dimension named above; an argument that names none is the same for every part. Nothing has to cross between parts.
All inputs are finite; a program needn't handle non-finite values.
Results may differ from the reference program's by a relative error of at most 0.0095.
The reference program's roundings to bfloat16 on the way (of `normed_in`, `query`, `weights`, `context`, `residual`, `normed_ffn` and `activated`) count: a program that leaves them out, or rounds other values in their place, can miss the bound.
Values may be sent and summed in bfloat16 or wider, within the bound.
No kernel may reach another device: no remote copies, remote signals or barrier semaphores. Data moves between devices by JAX's collectives and lax.ppermute only.
A program may use at most 128 MiB of HBM per device.

```python
import jax
import jax.numpy as jnp
from jax import lax

D = 4096
DH = 64
FF = 10240
H = 64
S = 2048
QLEN = 32
REQ = 8
TOK = 512


def kv_block(seed_key):
    width = 2 * H * DH
    base = jnp.clip(jax.random.normal(seed_key, (REQ, S, width), jnp.float32), -4.5, 4.5)
    return base.astype(jnp.bfloat16)


def draw_entering_kv(key, part):
    return kv_block(jax.random.fold_in(key, 11))


def draw_cached_kv(key, part):
    return kv_block(jax.random.fold_in(key, 23))


def place_ends(result, stream_key, smallest, top_value):
    longest = result.shape.index(max(result.shape))
    spots = []
    for shift in (0, 1):
        where = [jax.random.randint(jax.random.fold_in(stream_key, axis), (), 0, length) for axis, length in enumerate(result.shape)]
        where[longest] = (where[longest] + shift) % result.shape[longest]
        spots.append(tuple(where))
    return result.at[spots[0]].set(smallest).at[spots[1]].set(top_value)


def steps_of(own_key, extent, split, least, high):
    def one(dim, blocks):
        heights = jax.random.uniform(jax.random.fold_in(jax.random.fold_in(own_key, 6), dim), (blocks,), jnp.float32, least / len(split), high / len(split))
        return jnp.repeat(jnp.exp(heights), extent[dim] // blocks).reshape((-1,) + (1,) * (len(extent) - dim - 1))

    factor_of = one(*split[0])
    for cut in split[1:]:
        factor_of = factor_of * one(*cut)
    return factor_of


def gaussian(own_key, extent, scale, limit, pieces=(), kind=jnp.bfloat16):
    entries = jax.random.normal(own_key, extent, jnp.float32) * scale
    if len(pieces) > 0:
        entries = steps_of(own_key, extent, pieces, -0.22, 0.18) * entries
    return jnp.clip(entries, min=-limit, max=limit).astype(kind)


def setup_inputs(seed: int = 0, part: int = 0) -> dict:
    key_of = jax.random.split(jax.random.key(seed), 12)
    part_keys = jax.random.split(jax.random.fold_in(key_of[11], part), 12)
    hidden = gaussian(part_keys[0], (TOK, D), 1.0, 6.0, ((0, 64),))
    norm_gain_attn = jnp.clip(1.0 + 0.1 * jax.random.normal(key_of[1], (D,), jnp.float32), 0.5, 1.5)
    w_query = gaussian(key_of[2], (D, H * DH), D ** -0.5, 0.09375, ((1, 64),))
    entering_kv = draw_entering_kv(jax.random.fold_in(jax.random.fold_in(key_of[11], part), 71), part)
    cached_kv = draw_cached_kv(jax.random.fold_in(jax.random.fold_in(key_of[11], part), 71), part)
    enc_lengths = place_ends(jax.random.randint(part_keys[5], (2, REQ), S // 16, S + 1), jax.random.fold_in(part_keys[5], 1), S // 16, S).astype(jnp.int32)
    w_out = gaussian(key_of[6], (H * DH, D), (H * DH) ** -0.5, 0.09375, ((0, 64),))
    norm_gain_ffn = jnp.clip(1.0 + 0.1 * jax.random.normal(key_of[7], (D,), jnp.float32), 0.5, 1.5)
    w_gate = gaussian(key_of[8], (D, FF), D ** -0.5, 0.09375, ((1, 64),))
    w_up = gaussian(key_of[9], (D, FF), D ** -0.5, 0.09375, ((1, 64),))
    w_down = gaussian(key_of[10], (FF, D), FF ** -0.5, 0.0625, ((0, 64),))
    return {"hidden": hidden, "norm_gain_attn": norm_gain_attn, "w_query": w_query, "entering_kv": entering_kv, "cached_kv": cached_kv, "enc_lengths": enc_lengths, "w_out": w_out, "norm_gain_ffn": norm_gain_ffn, "w_gate": w_gate, "w_up": w_up, "w_down": w_down}


epsilon = 0.1

def normalize(matrix, gain_row):
    values = matrix.astype(jnp.float32)
    mean_square = lax.optimization_barrier(jnp.mean(values * values, axis=-1, keepdims=True))
    return (values * lax.rsqrt(mean_square + epsilon) * gain_row).astype(jnp.bfloat16)

def attend(query, key_value, lengths):
    requests = lengths.shape[0]
    head_count = key_value.shape[2] // (2 * DH)
    query_heads = query.reshape(requests, QLEN, head_count, DH).astype(jnp.float32)
    paired = key_value.reshape(requests, S, head_count, 2, DH).astype(jnp.float32)
    key_part = paired[:, :, :, 0, :]
    value_part = paired[:, :, :, 1, :]
    scores = jnp.einsum('rqhd,rshd->rhqs', query_heads, key_part)
    usable = (jnp.arange(S, dtype=jnp.int32)[None, :] < lengths[:, None].astype(jnp.int32))[:, None, None, :]
    masked = jnp.where(usable, scores, -1e+30)
    largest = lax.optimization_barrier(jnp.max(masked, axis=-1, keepdims=True))
    exponent = jnp.where(usable, jnp.exp(masked - largest), 0.0)
    weights = (exponent / lax.optimization_barrier(jnp.sum(exponent, axis=-1, keepdims=True))).astype(jnp.bfloat16)
    context = jnp.einsum('rhqs,rshd->rqhd', weights.astype(jnp.float32), value_part)
    return context.astype(jnp.bfloat16).reshape(requests * QLEN, head_count * DH)

def reference(hidden, norm_gain_attn, w_query, entering_kv, cached_kv, enc_lengths, w_out, norm_gain_ffn, w_gate, w_up, w_down):
    normed_in = normalize(hidden, norm_gain_attn)
    query = jnp.dot(normed_in, w_query, preferred_element_type=jnp.float32).astype(jnp.bfloat16)
    split_row = REQ * QLEN
    context = jnp.concatenate([attend(query[:split_row], entering_kv, enc_lengths[0]), attend(query[split_row:], cached_kv, enc_lengths[1])], axis=0)
    attention = jnp.dot(context, w_out, preferred_element_type=jnp.float32)
    residual = (hidden.astype(jnp.float32) + attention).astype(jnp.bfloat16)
    normed_ffn = normalize(residual, norm_gain_ffn)
    gate = jnp.dot(normed_ffn, w_gate, preferred_element_type=jnp.float32)
    upward = jnp.dot(normed_ffn, w_up, preferred_element_type=jnp.float32)
    activated = (jax.nn.gelu(gate, approximate=True) * upward).astype(jnp.bfloat16)
    return (residual.astype(jnp.float32) + jnp.dot(activated, w_down, preferred_element_type=jnp.float32)).astype(jnp.bfloat16)
```

```python
import jax
import jax.numpy as jnp
from jax import lax
from jax.experimental import pallas as pl
from jax.experimental.pallas import tpu as pltpu
from jax.sharding import Mesh
from jax.sharding import PartitionSpec as P

DH = 64
S = 2048
QLEN = 32
MP = ("mp_0", "mp_1")
GROUPS_MP = ("groups", "mp_0", "mp_1")
RING = 32
FAR = 8
NEG = -1e30
epsilon = 0.1

SLOTS = [(8 * k + (g if g < 5 else g - 8)) % RING for g in range(8) for k in range(4)]


def fetch(x, k):
    return lax.ppermute(x, "mp_0", [(i, (i - k) % RING) for i in range(RING)])


def other_core(x):
    return lax.ppermute(x, "mp_1", [(0, 1), (1, 0)])


def ring_gather(x):
    half = x.shape[1] // 2
    ahead = fetch(x, FAR)
    behind = fetch(x, -FAR)
    opposite = jnp.concatenate([fetch(ahead[:, :half], FAR), fetch(behind[:, half:], -FAR)], axis=1)
    here = jnp.stack([x, ahead, opposite, behind])
    right, left = [here], [here]
    for _ in range(3):
        right.append(fetch(right[-1], 1))
        left.append(fetch(left[-1], -1))
    right_last = fetch(right[3][:2], 1)
    left_last = fetch(jnp.concatenate([left[3][3:], left[3][:1]]), -1)
    return jnp.concatenate([*right, right_last, left_last, left[3], left[2], left[1]])


def ring_reduce(parts, join, finish, narrow):
    block = [parts[4 * g : 4 * g + 4] for g in range(8)]
    from_left = fetch(narrow(block[4][:2]), -1)
    from_right = fetch(narrow(block[4][2:]), 1)
    right = jnp.concatenate([join(block[3][:2], from_left), narrow(block[3][2:])])
    left = jnp.concatenate(
        [join(block[5][:1], from_right[1:]), narrow(block[5][1:3]), join(block[5][3:], from_right[:1])]
    )
    for step in (2, 1):
        right = join(block[step], fetch(right, -1))
        left = join(block[8 - step], fetch(left, 1))
    total = finish(block[0], fetch(right, -1), fetch(left, 1))
    half = total.shape[2] // 2
    ahead = fetch(narrow(total[2:3, :, :half]), -FAR)
    behind = fetch(narrow(total[2:3, :, half:]), FAR)
    to_ahead = jnp.concatenate(
        [join(total[1:2, :, :half], ahead), narrow(total[1:2, :, half:])], axis=2
    )
    to_behind = jnp.concatenate(
        [narrow(total[3:4, :, :half]), join(total[3:4, :, half:], behind)], axis=2
    )
    return total[0:1], fetch(to_ahead, -FAR), fetch(to_behind, FAR)


def narrow_sum(x):
    return x.astype(jnp.bfloat16)


def join_sum(mine, arrived):
    return (mine.astype(jnp.float32) + arrived.astype(jnp.float32)).astype(jnp.bfloat16)


def add_three(mine, one, two):
    return mine.astype(jnp.float32) + (one.astype(jnp.float32) + two.astype(jnp.float32))


def sum_over_ring(parts):
    return add_three(*ring_reduce(parts, join_sum, add_three, narrow_sum))[0]


def normalize(matrix, gain_row):
    values = matrix.astype(jnp.float32)
    mean_square = jnp.mean(values * values, axis=-1, keepdims=True)
    return (values * lax.rsqrt(mean_square + epsilon) * gain_row).astype(jnp.bfloat16)


def attend(query, key_value, lengths):
    requests = lengths.shape[0]
    head_count = key_value.shape[2] // (2 * DH)
    query_heads = query.reshape(requests, QLEN, head_count, DH)
    paired = key_value.reshape(requests, S, head_count, 2, DH)
    key_part = paired[:, :, :, 0, :]
    value_part = paired[:, :, :, 1, :]
    scores = jnp.einsum(
        "rqhd,rshd->rhqs", query_heads, key_part, preferred_element_type=jnp.float32
    )
    usable = (jnp.arange(S, dtype=jnp.int32)[None, :] < lengths[:, None])[:, None, None, :]
    masked = jnp.where(usable, scores, NEG)
    largest = jnp.max(masked, axis=-1, keepdims=True)
    exponent = jnp.where(usable, jnp.exp(masked - largest), 0.0)
    weights = (exponent / jnp.sum(exponent, axis=-1, keepdims=True)).astype(jnp.bfloat16)
    context = jnp.einsum("rhqs,rshd->rqhd", weights, value_part, preferred_element_type=jnp.float32)
    return context.astype(jnp.bfloat16).reshape(requests * QLEN, head_count * DH)


def every_second_head(key_value, parity):
    requests, positions, width = key_value.shape
    heads = width // (2 * 2 * DH)
    together = 4
    lane = 2 * DH

    def body(parity_ref, *refs):
        for j in range(together):
            refs[together][:, :, j * lane : (j + 1) * lane] = refs[j][...]

    def column(j):
        return lambda i, p: (0, 0, 2 * (together * i + j) + p[0])

    return pl.pallas_call(
        body,
        grid_spec=pltpu.PrefetchScalarGridSpec(
            num_scalar_prefetch=1,
            grid=(heads // together,),
            in_specs=[pl.BlockSpec((requests, positions, lane), column(j)) for j in range(together)],
            out_specs=pl.BlockSpec((requests, positions, together * lane), lambda i, p: (0, 0, i)),
        ),
        out_shape=jax.ShapeDtypeStruct((requests, positions, heads * lane), key_value.dtype),
        name="every_second_head",
    )(parity, *([key_value] * together))


def split_rows(value):
    high = value.astype(jnp.bfloat16)
    rest = value - high.astype(jnp.float32)
    middle = rest.astype(jnp.bfloat16)
    low = (rest - middle.astype(jnp.float32)).astype(jnp.bfloat16)
    return [high, middle, low]


def pack(sums, largest, weight):
    rows = split_rows(largest) + split_rows(weight)
    zero = jnp.zeros((10, sums.shape[1]), jnp.float32)
    tail = jnp.concatenate([r.astype(jnp.float32) for r in rows] + [zero], axis=0)
    return jnp.concatenate([sums.astype(jnp.bfloat16), tail.astype(jnp.bfloat16)], axis=0)


def unpack(part):
    sums = part[:DH].astype(jnp.float32)
    tail = part[DH:].astype(jnp.float32)
    return sums, tail[0:1] + tail[1:2] + tail[2:3], tail[3:4] + tail[4:5] + tail[5:6]


def merge(first, second):
    sums_a, largest_a, weight_a = first
    sums_b, largest_b, weight_b = second
    largest = jnp.maximum(largest_a, largest_b)
    scale_a = jnp.exp(largest_a - largest)
    scale_b = jnp.exp(largest_b - largest)
    return (
        sums_a * scale_a + sums_b * scale_b,
        largest,
        weight_a * scale_a + weight_b * scale_b,
    )


def partial_attention(query, own, partner, usable, columns):
    count, _, tokens = query.shape
    requests, positions, _ = own.shape
    lane = 2 * DH
    rows = requests * positions

    def body(columns_ref, q_ref, own_ref, partner_ref, usable_ref, out_ref):
        kv = jnp.concatenate(
            [own_ref[...].reshape(rows, lane), partner_ref[...].reshape(rows, lane)], axis=0
        )
        q = jnp.concatenate([q_ref[0], jnp.zeros((DH, tokens), jnp.bfloat16)], axis=0)
        kept = usable_ref[...] > 0.5
        scores = jnp.dot(kv, q, preferred_element_type=jnp.float32)
        scores = jnp.where(kept, scores, NEG)
        largest = jnp.max(scores, axis=0, keepdims=True)
        exponent = jnp.where(kept, jnp.exp(scores - largest), 0.0)
        weight = jnp.sum(exponent, axis=0, keepdims=True)
        sums = lax.dot_general(
            kv, exponent.astype(jnp.bfloat16), (((0,), (0,)), ((), ())),
            preferred_element_type=jnp.float32,
        )
        out_ref[0] = pack(sums[DH:], largest, weight)

    return pl.pallas_call(
        body,
        grid_spec=pltpu.PrefetchScalarGridSpec(
            num_scalar_prefetch=1,
            grid=(count,),
            in_specs=[
                pl.BlockSpec((1, DH, tokens), lambda i, c: (i, 0, 0)),
                pl.BlockSpec((requests, positions, lane), lambda i, c: (0, 0, c[0, i])),
                pl.BlockSpec((requests, positions, lane), lambda i, c: (0, 0, c[1, i])),
                pl.BlockSpec((2 * rows, tokens), lambda i, c: (0, 0)),
            ],
            out_specs=pl.BlockSpec((1, DH + 16, tokens), lambda i, c: (i, 0, 0)),
        ),
        out_shape=jax.ShapeDtypeStruct((count, DH + 16, tokens), jnp.bfloat16),
        name="partial_attention",
    )(columns, query, own, partner, usable)


def join_parts(*parts):
    def body(*refs):
        for n in range(parts[0].shape[0]):
            total = unpack(refs[0][n])
            for ref in refs[1:-1]:
                total = merge(total, unpack(ref[n]))
            refs[-1][n] = pack(*total)

    return pl.pallas_call(
        body, out_shape=jax.ShapeDtypeStruct(parts[0].shape, jnp.bfloat16), name="join_parts"
    )(*parts)


def close_parts(*parts):
    def body(*refs):
        total = unpack(refs[0][0])
        for ref in refs[1:-1]:
            total = merge(total, unpack(ref[0]))
        sums, _, weight = total
        refs[-1][...] = (sums / weight).astype(jnp.bfloat16)

    return pl.pallas_call(
        body,
        out_shape=jax.ShapeDtypeStruct((DH, parts[0].shape[2]), jnp.bfloat16),
        name="close_parts",
    )(*parts)


def token_order(tokens, chip, core):
    n = lax.broadcasted_iota(jnp.int32, (tokens, tokens), 1)
    m = lax.broadcasted_iota(jnp.int32, (tokens, tokens), 0)
    each = tokens // (2 * RING)
    slot = (n // (2 * each) - chip + RING) % RING
    near = slot % 8
    far = (slot // 8 + (near >= 5)) % 4
    half = ((n // each) % 2 != core).astype(jnp.int32)
    row = half * (tokens // 2) + (near * 4 + far) * each + n % each
    return (row == m).astype(jnp.bfloat16)


def per_device(
    hidden,
    norm_gain_attn,
    w_query,
    entering_kv,
    cached_kv,
    enc_lengths,
    w_out,
    norm_gain_ffn,
    w_gate,
    w_up,
    w_down,
):
    chip = lax.axis_index("mp_0").astype(jnp.int32)
    core = lax.axis_index("mp_1").astype(jnp.int32)
    rows, width = hidden.shape
    mine = RING * rows
    tokens = 2 * mine
    requests, positions, _ = entering_kv.shape

    partner_kv = other_core(every_second_head(entering_kv, (1 - core)[None]))
    order = token_order(tokens, chip, core)
    entered = tokens // 2
    place = jnp.arange(2 * requests * positions, dtype=jnp.int32)
    source = jnp.where(place // (requests * positions) == 0, core, 1 - core)
    at = (2 * chip + source) * positions + place % positions
    row_request = (place // positions) % requests
    in_length = at < jnp.take(enc_lengths[0], row_request)
    token_request = jnp.arange(entered, dtype=jnp.int32) // QLEN
    usable = (
        (row_request[:, None] == token_request[None, :]) & in_length[:, None]
    ).astype(jnp.float32)
    heads = (chip + jnp.array(SLOTS, jnp.int32)) % RING
    columns = jnp.stack([2 * heads + core, heads])

    def everyone(x):
        gathered = ring_gather(x).reshape(mine, width)
        return gathered, other_core(gathered)

    def query_of(x):
        return lax.dot_general(
            w_query, x, (((0,), (1,)), ((), ())), preferred_element_type=jnp.float32
        ).astype(jnp.bfloat16)

    normed_own, normed_other = everyone(normalize(hidden, norm_gain_attn))
    query = jnp.concatenate([query_of(normed_own), query_of(normed_other)], axis=1)
    query = jnp.dot(query, order, preferred_element_type=jnp.float32).astype(jnp.bfloat16)

    gathered_query = ring_gather(query[:, :entered])
    parts = partial_attention(gathered_query, entering_kv, partner_kv, usable, columns)
    context_entering = close_parts(*ring_reduce(parts, join_parts, join_parts, lambda x: x))
    context_cached = attend(query[:, entered:].T, cached_kv, enc_lengths[1]).T
    context = jnp.concatenate([context_entering, context_cached], axis=1)
    context = lax.dot_general(
        context, order, (((1,), (1,)), ((), ())), preferred_element_type=jnp.float32
    ).astype(jnp.bfloat16)

    def summed(product_of, own, other):
        arrived = other_core(product_of(other).astype(jnp.bfloat16))
        total = product_of(own) + arrived.astype(jnp.float32)
        return sum_over_ring(total.reshape(RING, rows, width))

    def out_product(x):
        return lax.dot_general(
            x, w_out, (((0,), (0,)), ((), ())), preferred_element_type=jnp.float32
        )

    attention = summed(out_product, context[:, :mine], context[:, mine:])
    residual = (hidden.astype(jnp.float32) + attention).astype(jnp.bfloat16)

    def feed(x):
        gate = jnp.dot(x, w_gate, preferred_element_type=jnp.float32)
        upward = jnp.dot(x, w_up, preferred_element_type=jnp.float32)
        activated = (jax.nn.gelu(gate, approximate=True) * upward).astype(jnp.bfloat16)
        return jnp.dot(activated, w_down, preferred_element_type=jnp.float32)

    feed_out = summed(feed, *everyone(normalize(residual, norm_gain_ffn)))
    return (residual.astype(jnp.float32) + feed_out).astype(jnp.bfloat16)


def solution(mesh):
    torus = Mesh(mesh.devices.reshape(mesh.shape["groups"], RING, 2), ("groups", "mp_0", "mp_1"))
    in_specs = (
        P(GROUPS_MP, None),
        P(),
        P(None, MP),
        P("groups", MP, None),
        P("groups", None, MP),
        P(None, "groups"),
        P(MP, None),
        P(),
        P(None, MP),
        P(None, MP),
        P(MP, None),
    )
    out_specs = P(GROUPS_MP, None)
    return jax.shard_map(
        per_device, mesh=torus, in_specs=in_specs, out_specs=out_specs, check_vma=False
    )
```

```python
import jax
import jax.numpy as jnp
from jax import lax
from jax.experimental import pallas as pl
from jax.experimental.pallas import tpu as pltpu
from jax.sharding import Mesh
from jax.sharding import PartitionSpec as P

DH = 64
S = 2048
QLEN = 32
MP = ("mp_0", "mp_1")
GROUPS_MP = ("groups", "mp_0", "mp_1")
RING = 32
FAR = 8
NEG = -1e30
epsilon = 0.1

SLOTS = [(8 * k + (g if g < 5 else g - 8)) % RING for g in range(8) for k in range(4)]


def fetch(x, k):
    return lax.ppermute(x, "mp_0", [(i, (i - k) % RING) for i in range(RING)])


def other_core(x):
    return lax.ppermute(x, "mp_1", [(0, 1), (1, 0)])


def ring_gather(x, meanwhile=()):
    half = x.shape[1] // 2
    ahead = fetch(x, FAR)
    behind = fetch(x, -FAR)
    opposite = jnp.concatenate([fetch(ahead[:, :half], FAR), fetch(behind[:, half:], -FAR)], axis=1)
    here, meanwhile = lax.optimization_barrier(
        (jnp.stack([x, ahead, opposite, behind]), meanwhile)
    )
    right, left = [here], [here]
    for _ in range(3):
        right.append(fetch(right[-1], 1))
        left.append(fetch(left[-1], -1))
    right_last = fetch(right[3][:2], 1)
    left_last = fetch(jnp.concatenate([left[3][3:], left[3][:1]]), -1)
    gathered = jnp.concatenate([*right, right_last, left_last, left[3], left[2], left[1]])
    return gathered, meanwhile


def ring_reduce(parts, join, finish, narrow):
    block = [parts[4 * g : 4 * g + 4] for g in range(8)]
    from_left = fetch(narrow(block[4][:2]), -1)
    from_right = fetch(narrow(block[4][2:]), 1)
    right = jnp.concatenate([join(block[3][:2], from_left), narrow(block[3][2:])])
    left = jnp.concatenate(
        [join(block[5][:1], from_right[1:]), narrow(block[5][1:3]), join(block[5][3:], from_right[:1])]
    )
    for step in (2, 1):
        right = join(block[step], fetch(right, -1))
        left = join(block[8 - step], fetch(left, 1))
    total = finish(block[0], fetch(right, -1), fetch(left, 1))
    half = total.shape[2] // 2
    ahead = fetch(narrow(total[2:3, :, :half]), -FAR)
    behind = fetch(narrow(total[2:3, :, half:]), FAR)
    to_ahead = jnp.concatenate(
        [join(total[1:2, :, :half], ahead), narrow(total[1:2, :, half:])], axis=2
    )
    to_behind = jnp.concatenate(
        [narrow(total[3:4, :, :half]), join(total[3:4, :, half:], behind)], axis=2
    )
    return total[0:1], fetch(to_ahead, -FAR), fetch(to_behind, FAR)


def narrow_sum(x):
    return x.astype(jnp.bfloat16)


def join_sum(mine, arrived):
    return (mine.astype(jnp.float32) + arrived.astype(jnp.float32)).astype(jnp.bfloat16)


def add_three(mine, one, two):
    return mine.astype(jnp.float32) + (one.astype(jnp.float32) + two.astype(jnp.float32))


def sum_over_ring(parts):
    return add_three(*ring_reduce(parts, join_sum, add_three, narrow_sum))[0]


def normalize(matrix, gain_row):
    values = matrix.astype(jnp.float32)
    mean_square = jnp.mean(values * values, axis=-1, keepdims=True)
    return (values * lax.rsqrt(mean_square + epsilon) * gain_row).astype(jnp.bfloat16)


def attend(query, key_value, lengths):
    requests = lengths.shape[0]
    head_count = key_value.shape[2] // (2 * DH)
    query_heads = query.reshape(requests, QLEN, head_count, DH)
    paired = key_value.reshape(requests, S, head_count, 2, DH)
    key_part = paired[:, :, :, 0, :]
    value_part = paired[:, :, :, 1, :]
    scores = jnp.einsum(
        "rqhd,rshd->rhqs", query_heads, key_part, preferred_element_type=jnp.float32
    )
    usable = (jnp.arange(S, dtype=jnp.int32)[None, :] < lengths[:, None])[:, None, None, :]
    masked = jnp.where(usable, scores, NEG)
    largest = jnp.max(masked, axis=-1, keepdims=True)
    exponent = jnp.where(usable, jnp.exp(masked - largest), 0.0)
    weights = (exponent / jnp.sum(exponent, axis=-1, keepdims=True)).astype(jnp.bfloat16)
    context = jnp.einsum("rhqs,rshd->rqhd", weights, value_part, preferred_element_type=jnp.float32)
    return context.astype(jnp.bfloat16).reshape(requests * QLEN, head_count * DH)


def every_second_head(key_value, parity):
    requests, positions, width = key_value.shape
    heads = width // (2 * 2 * DH)
    together = 4
    lane = 2 * DH

    def body(parity_ref, *refs):
        for j in range(together):
            refs[together][:, :, j * lane : (j + 1) * lane] = refs[j][...]

    def column(j):
        return lambda i, p: (0, 0, 2 * (together * i + j) + p[0])

    return pl.pallas_call(
        body,
        grid_spec=pltpu.PrefetchScalarGridSpec(
            num_scalar_prefetch=1,
            grid=(heads // together,),
            in_specs=[pl.BlockSpec((requests, positions, lane), column(j)) for j in range(together)],
            out_specs=pl.BlockSpec((requests, positions, together * lane), lambda i, p: (0, 0, i)),
        ),
        out_shape=jax.ShapeDtypeStruct((requests, positions, heads * lane), key_value.dtype),
        name="every_second_head",
    )(parity, *([key_value] * together))


def split_rows(value):
    high = value.astype(jnp.bfloat16)
    rest = value - high.astype(jnp.float32)
    middle = rest.astype(jnp.bfloat16)
    low = (rest - middle.astype(jnp.float32)).astype(jnp.bfloat16)
    return [high, middle, low]


def pack(sums, largest, weight):
    rows = split_rows(largest) + split_rows(weight)
    zero = jnp.zeros((10, sums.shape[1]), jnp.float32)
    tail = jnp.concatenate([r.astype(jnp.float32) for r in rows] + [zero], axis=0)
    return jnp.concatenate([sums.astype(jnp.bfloat16), tail.astype(jnp.bfloat16)], axis=0)


def unpack(part):
    sums = part[:DH].astype(jnp.float32)
    tail = part[DH:].astype(jnp.float32)
    return sums, tail[0:1] + tail[1:2] + tail[2:3], tail[3:4] + tail[4:5] + tail[5:6]


def merge(first, second):
    sums_a, largest_a, weight_a = first
    sums_b, largest_b, weight_b = second
    largest = jnp.maximum(largest_a, largest_b)
    scale_a = jnp.exp(largest_a - largest)
    scale_b = jnp.exp(largest_b - largest)
    return (
        sums_a * scale_a + sums_b * scale_b,
        largest,
        weight_a * scale_a + weight_b * scale_b,
    )


def partial_attention(query, own, partner, usable, columns):
    count, _, tokens = query.shape
    requests, positions, _ = own.shape
    lane = 2 * DH
    groups, rows, together = usable.shape
    each = requests // groups

    def body(columns_ref, q_ref, own_ref, partner_ref, usable_ref, out_ref):
        for g in range(groups):
            some = slice(g * each, (g + 1) * each)
            lanes = slice(g * together, (g + 1) * together)
            kv = jnp.concatenate(
                [ref[some].reshape(rows // 2, lane) for ref in (own_ref, partner_ref)], axis=0
            )
            q = jnp.concatenate(
                [q_ref[0, :, lanes], jnp.zeros((DH, together), jnp.bfloat16)], axis=0
            )
            kept = usable_ref[g] > 0.5
            scores = jnp.dot(kv, q, preferred_element_type=jnp.float32)
            scores = jnp.where(kept, scores, NEG)
            largest = jnp.max(scores, axis=0, keepdims=True)
            exponent = jnp.where(kept, jnp.exp(scores - largest), 0.0)
            weight = jnp.sum(exponent, axis=0, keepdims=True)
            sums = lax.dot_general(
                kv, exponent.astype(jnp.bfloat16), (((0,), (0,)), ((), ())),
                preferred_element_type=jnp.float32,
            )
            out_ref[0, :, lanes] = pack(sums[DH:], largest, weight)

    return pl.pallas_call(
        body,
        grid_spec=pltpu.PrefetchScalarGridSpec(
            num_scalar_prefetch=1,
            grid=(count,),
            in_specs=[
                pl.BlockSpec((1, DH, tokens), lambda i, c: (i, 0, 0)),
                pl.BlockSpec((requests, positions, lane), lambda i, c: (0, 0, c[0, i])),
                pl.BlockSpec((requests, positions, lane), lambda i, c: (0, 0, c[1, i])),
                pl.BlockSpec(usable.shape, lambda i, c: (0, 0, 0)),
            ],
            out_specs=pl.BlockSpec((1, DH + 16, tokens), lambda i, c: (i, 0, 0)),
        ),
        out_shape=jax.ShapeDtypeStruct((count, DH + 16, tokens), jnp.bfloat16),
        name="partial_attention",
    )(columns, query, own, partner, usable)


def join_parts(*parts):
    def body(*refs):
        for n in range(parts[0].shape[0]):
            total = unpack(refs[0][n])
            for ref in refs[1:-1]:
                total = merge(total, unpack(ref[n]))
            refs[-1][n] = pack(*total)

    return pl.pallas_call(
        body, out_shape=jax.ShapeDtypeStruct(parts[0].shape, jnp.bfloat16), name="join_parts"
    )(*parts)


def close_parts(*parts):
    def body(*refs):
        total = unpack(refs[0][0])
        for ref in refs[1:-1]:
            total = merge(total, unpack(ref[0]))
        sums, _, weight = total
        refs[-1][...] = (sums / weight).astype(jnp.bfloat16)

    return pl.pallas_call(
        body,
        out_shape=jax.ShapeDtypeStruct((DH, parts[0].shape[2]), jnp.bfloat16),
        name="close_parts",
    )(*parts)


def token_order(tokens, chip, core):
    n = lax.broadcasted_iota(jnp.int32, (tokens, tokens), 1)
    m = lax.broadcasted_iota(jnp.int32, (tokens, tokens), 0)
    each = tokens // (2 * RING)
    slot = (n // (2 * each) - chip + RING) % RING
    near = slot % 8
    far = (slot // 8 + (near >= 5)) % 4
    half = ((n // each) % 2 != core).astype(jnp.int32)
    row = half * (tokens // 2) + (near * 4 + far) * each + n % each
    return (row == m).astype(jnp.bfloat16)


def per_device(
    hidden,
    norm_gain_attn,
    w_query,
    entering_kv,
    cached_kv,
    enc_lengths,
    w_out,
    norm_gain_ffn,
    w_gate,
    w_up,
    w_down,
):
    chip = lax.axis_index("mp_0").astype(jnp.int32)
    core = lax.axis_index("mp_1").astype(jnp.int32)
    rows, width = hidden.shape
    mine = RING * rows
    tokens = 2 * mine
    requests, positions, _ = entering_kv.shape

    partner_kv = other_core(every_second_head(entering_kv, (1 - core)[None]))
    partner_weights = [other_core(w) for w in (w_query, w_out, w_gate, w_up, w_down)]
    order = token_order(tokens, chip, core)
    entered = tokens // 2
    groups = max(1, entered // 128)
    each = requests // groups
    mask_shape = (groups, 2 * each * positions, entered // groups)
    row = lax.broadcasted_iota(jnp.int32, mask_shape, 1)
    source = jnp.where(row // (each * positions) == 0, core, 1 - core)
    at = (2 * chip + source) * positions + row % positions
    lengths = jnp.broadcast_to(
        enc_lengths[0].reshape(groups, 1, each, 1), (groups, 2, each, positions)
    ).reshape(mask_shape[:2])
    same = (row // positions) % each == lax.broadcasted_iota(jnp.int32, mask_shape, 2) // QLEN
    usable = (same & (at < lengths[:, :, None])).astype(jnp.float32)
    heads = (chip + jnp.array(SLOTS, jnp.int32)) % RING
    columns = jnp.stack([2 * heads + core, heads])

    def query_of(w, x):
        return lax.dot_general(
            w, x, (((0,), (1,)), ((), ())), preferred_element_type=jnp.float32
        ).astype(jnp.bfloat16)

    normed, (partner_kv, partner_weights, order, usable, columns) = ring_gather(
        normalize(hidden, norm_gain_attn), (partner_kv, partner_weights, order, usable, columns)
    )
    normed = normed.reshape(mine, width)
    query_p, out_p, gate_p, up_p, down_p = partner_weights
    arrived = other_core(query_of(query_p, normed))
    query = jnp.concatenate([query_of(w_query, normed), arrived], axis=1)
    query = jnp.dot(query, order, preferred_element_type=jnp.float32).astype(jnp.bfloat16)

    gathered_query, _ = ring_gather(query[:, :entered])
    parts = partial_attention(gathered_query, entering_kv, partner_kv, usable, columns)
    context_entering = close_parts(*ring_reduce(parts, join_parts, join_parts, lambda x: x))
    context_cached = attend(query[:, entered:].T, cached_kv, enc_lengths[1]).T
    context = jnp.concatenate([context_entering, context_cached], axis=1)
    context = lax.dot_general(
        context, order, (((1,), (1,)), ((), ())), preferred_element_type=jnp.float32
    ).astype(jnp.bfloat16)

    def out_product(x, w):
        return lax.dot_general(x, w, (((0,), (0,)), ((), ())), preferred_element_type=jnp.float32)

    arrived = other_core(context[:, mine:])
    product = out_product(context[:, :mine], w_out) + out_product(arrived, out_p)
    attention = sum_over_ring(product.reshape(RING, rows, width))
    residual = (hidden.astype(jnp.float32) + attention).astype(jnp.bfloat16)

    def feed(x, gate_w, up_w, down_w):
        gate = jnp.dot(x, gate_w, preferred_element_type=jnp.float32)
        upward = jnp.dot(x, up_w, preferred_element_type=jnp.float32)
        activated = (jax.nn.gelu(gate, approximate=True) * upward).astype(jnp.bfloat16)
        return jnp.dot(activated, down_w, preferred_element_type=jnp.float32)

    normed, _ = ring_gather(normalize(residual, norm_gain_ffn))
    normed = normed.reshape(mine, width)
    product = feed(normed, w_gate, w_up, w_down) + feed(normed, gate_p, up_p, down_p)
    feed_out = sum_over_ring(product.reshape(RING, rows, width))
    return (residual.astype(jnp.float32) + feed_out).astype(jnp.bfloat16)


def solution(mesh):
    torus = Mesh(mesh.devices.reshape(mesh.shape["groups"], RING, 2), ("groups", "mp_0", "mp_1"))
    in_specs = (
        P(GROUPS_MP, None),
        P(),
        P(None, MP),
        P("groups", MP, None),
        P("groups", None, MP),
        P(None, "groups"),
        P(MP, None),
        P(),
        P(None, MP),
        P(None, MP),
        P(MP, None),
    )
    out_specs = P(GROUPS_MP, None)
    return jax.shard_map(
        per_device, mesh=torus, in_specs=in_specs, out_specs=out_specs, check_vma=False
    )
```

```python
import jax
import jax.numpy as jnp
from jax import lax
from jax.experimental import pallas as pl
from jax.experimental.pallas import tpu as pltpu
from jax.sharding import Mesh
from jax.sharding import PartitionSpec as P

DH = 64
S = 2048
QLEN = 32
MP = ("mp_0", "mp_1")
GROUPS_MP = ("groups", "mp_0", "mp_1")
RING = 32
FAR = 8
NEG = -1e30
epsilon = 0.1

SLOTS = [(8 * k + (g if g < 5 else g - 8)) % RING for g in range(8) for k in range(4)]


def fetch(x, k):
    return lax.ppermute(x, "mp_0", [(i, (i - k) % RING) for i in range(RING)])


def other_core(x):
    return lax.ppermute(x, "mp_1", [(0, 1), (1, 0)])


def ring_gather(x, meanwhile=()):
    ahead = fetch(x, FAR)
    behind = fetch(x, -FAR)
    opposite = fetch(ahead, FAR)
    here, meanwhile = lax.optimization_barrier(
        (jnp.stack([x, ahead, opposite, behind]), meanwhile)
    )
    right, left = [here], [here]
    for _ in range(3):
        right.append(fetch(right[-1], 1))
        left.append(fetch(left[-1], -1))
    right.append(fetch(right[-1], 1))
    gathered = jnp.concatenate([*right, left[3], left[2], left[1]])
    return gathered, meanwhile


def ring_reduce(parts, join, finish, narrow):
    block = [parts[4 * g : 4 * g + 4] for g in range(8)]
    right, left = join(block[3], fetch(narrow(block[4]), -1)), narrow(block[5])
    for step in (2, 1):
        right = join(block[step], fetch(right, -1))
        left = join(block[8 - step], fetch(left, 1))
    total = finish(block[0], fetch(right, -1), fetch(left, 1))
    opposite = fetch(narrow(total[2:3]), -FAR)
    behind = fetch(narrow(total[3:4]), FAR)
    return total[0:1], fetch(join(total[1:2], opposite), -FAR), behind


def narrow_sum(x):
    return x.astype(jnp.bfloat16)


def join_sum(mine, arrived):
    return (mine.astype(jnp.float32) + arrived.astype(jnp.float32)).astype(jnp.bfloat16)


def add_three(mine, one, two):
    return mine.astype(jnp.float32) + (one.astype(jnp.float32) + two.astype(jnp.float32))


def sum_over_ring(parts):
    return add_three(*ring_reduce(parts, join_sum, add_three, narrow_sum))[0]


def normalize(matrix, gain_row):
    values = matrix.astype(jnp.float32)
    mean_square = jnp.mean(values * values, axis=-1, keepdims=True)
    return (values * lax.rsqrt(mean_square + epsilon) * gain_row).astype(jnp.bfloat16)


def attend(query, key_value, lengths):
    requests = lengths.shape[0]
    head_count = key_value.shape[2] // (2 * DH)
    query_heads = query.reshape(requests, QLEN, head_count, DH)
    paired = key_value.reshape(requests, S, head_count, 2, DH)
    key_part = paired[:, :, :, 0, :]
    value_part = paired[:, :, :, 1, :]
    scores = jnp.einsum(
        "rqhd,rshd->rhqs", query_heads, key_part, preferred_element_type=jnp.float32
    )
    usable = (jnp.arange(S, dtype=jnp.int32)[None, :] < lengths[:, None])[:, None, None, :]
    masked = jnp.where(usable, scores, NEG)
    largest = jnp.max(masked, axis=-1, keepdims=True)
    exponent = jnp.where(usable, jnp.exp(masked - largest), 0.0)
    weights = (exponent / jnp.sum(exponent, axis=-1, keepdims=True)).astype(jnp.bfloat16)
    context = jnp.einsum("rhqs,rshd->rqhd", weights, value_part, preferred_element_type=jnp.float32)
    return context.astype(jnp.bfloat16).reshape(requests * QLEN, head_count * DH)


def every_second_head(key_value, parity):
    requests, positions, width = key_value.shape
    heads = width // (2 * 2 * DH)
    together = 4
    lane = 2 * DH

    def body(parity_ref, *refs):
        for j in range(together):
            refs[together][:, :, j * lane : (j + 1) * lane] = refs[j][...]

    def column(j):
        return lambda i, p: (0, 0, 2 * (together * i + j) + p[0])

    return pl.pallas_call(
        body,
        grid_spec=pltpu.PrefetchScalarGridSpec(
            num_scalar_prefetch=1,
            grid=(heads // together,),
            in_specs=[pl.BlockSpec((requests, positions, lane), column(j)) for j in range(together)],
            out_specs=pl.BlockSpec((requests, positions, together * lane), lambda i, p: (0, 0, i)),
        ),
        out_shape=jax.ShapeDtypeStruct((requests, positions, heads * lane), key_value.dtype),
        name="every_second_head",
    )(parity, *([key_value] * together))


def split_rows(value):
    high = value.astype(jnp.bfloat16)
    rest = value - high.astype(jnp.float32)
    middle = rest.astype(jnp.bfloat16)
    low = (rest - middle.astype(jnp.float32)).astype(jnp.bfloat16)
    return [high, middle, low]


def pack(sums, largest, weight):
    rows = split_rows(largest) + split_rows(weight)
    zero = jnp.zeros((10, sums.shape[1]), jnp.float32)
    tail = jnp.concatenate([r.astype(jnp.float32) for r in rows] + [zero], axis=0)
    return jnp.concatenate([sums.astype(jnp.bfloat16), tail.astype(jnp.bfloat16)], axis=0)


def unpack(part):
    sums = part[:DH].astype(jnp.float32)
    tail = part[DH:].astype(jnp.float32)
    return sums, tail[0:1] + tail[1:2] + tail[2:3], tail[3:4] + tail[4:5] + tail[5:6]


def merge(first, second):
    sums_a, largest_a, weight_a = first
    sums_b, largest_b, weight_b = second
    largest = jnp.maximum(largest_a, largest_b)
    scale_a = jnp.exp(largest_a - largest)
    scale_b = jnp.exp(largest_b - largest)
    return (
        sums_a * scale_a + sums_b * scale_b,
        largest,
        weight_a * scale_a + weight_b * scale_b,
    )


def partial_attention(query, own, partner, usable, columns):
    count, _, tokens = query.shape
    requests, positions, _ = own.shape
    lane = 2 * DH
    groups, rows, together = usable.shape
    each = requests // groups

    def body(columns_ref, q_ref, own_ref, partner_ref, usable_ref, out_ref):
        for g in range(groups):
            some = slice(g * each, (g + 1) * each)
            lanes = slice(g * together, (g + 1) * together)
            kv = jnp.concatenate(
                [ref[some].reshape(rows // 2, lane) for ref in (own_ref, partner_ref)], axis=0
            )
            q = jnp.concatenate(
                [q_ref[0, :, lanes], jnp.zeros((DH, together), jnp.bfloat16)], axis=0
            )
            kept = usable_ref[g] > 0.5
            scores = jnp.dot(kv, q, preferred_element_type=jnp.float32)
            scores = jnp.where(kept, scores, NEG)
            largest = jnp.max(scores, axis=0, keepdims=True)
            exponent = jnp.where(kept, jnp.exp(scores - largest), 0.0)
            weight = jnp.sum(exponent, axis=0, keepdims=True)
            sums = lax.dot_general(
                kv, exponent.astype(jnp.bfloat16), (((0,), (0,)), ((), ())),
                preferred_element_type=jnp.float32,
            )
            out_ref[0, :, lanes] = pack(sums[DH:], largest, weight)

    return pl.pallas_call(
        body,
        grid_spec=pltpu.PrefetchScalarGridSpec(
            num_scalar_prefetch=1,
            grid=(count,),
            in_specs=[
                pl.BlockSpec((1, DH, tokens), lambda i, c: (i, 0, 0)),
                pl.BlockSpec((requests, positions, lane), lambda i, c: (0, 0, c[0, i])),
                pl.BlockSpec((requests, positions, lane), lambda i, c: (0, 0, c[1, i])),
                pl.BlockSpec(usable.shape, lambda i, c: (0, 0, 0)),
            ],
            out_specs=pl.BlockSpec((1, DH + 16, tokens), lambda i, c: (i, 0, 0)),
        ),
        out_shape=jax.ShapeDtypeStruct((count, DH + 16, tokens), jnp.bfloat16),
        name="partial_attention",
    )(columns, query, own, partner, usable)


def join_parts(*parts):
    def body(*refs):
        for n in range(parts[0].shape[0]):
            total = unpack(refs[0][n])
            for ref in refs[1:-1]:
                total = merge(total, unpack(ref[n]))
            refs[-1][n] = pack(*total)

    return pl.pallas_call(
        body, out_shape=jax.ShapeDtypeStruct(parts[0].shape, jnp.bfloat16), name="join_parts"
    )(*parts)


def close_parts(*parts):
    def body(*refs):
        total = unpack(refs[0][0])
        for ref in refs[1:-1]:
            total = merge(total, unpack(ref[0]))
        sums, _, weight = total
        refs[-1][...] = (sums / weight).astype(jnp.bfloat16)

    return pl.pallas_call(
        body,
        out_shape=jax.ShapeDtypeStruct((DH, parts[0].shape[2]), jnp.bfloat16),
        name="close_parts",
    )(*parts)


def token_order(tokens, chip, core):
    n = lax.broadcasted_iota(jnp.int32, (tokens, tokens), 1)
    m = lax.broadcasted_iota(jnp.int32, (tokens, tokens), 0)
    each = tokens // (2 * RING)
    slot = (n // (2 * each) - chip + RING) % RING
    near = slot % 8
    far = (slot // 8 + (near >= 5)) % 4
    half = ((n // each) % 2 != core).astype(jnp.int32)
    row = half * (tokens // 2) + (near * 4 + far) * each + n % each
    return (row == m).astype(jnp.bfloat16)


def per_device(
    hidden,
    norm_gain_attn,
    w_query,
    entering_kv,
    cached_kv,
    enc_lengths,
    w_out,
    norm_gain_ffn,
    w_gate,
    w_up,
    w_down,
):
    chip = lax.axis_index("mp_0").astype(jnp.int32)
    core = lax.axis_index("mp_1").astype(jnp.int32)
    rows, width = hidden.shape
    mine = RING * rows
    tokens = 2 * mine
    requests, positions, _ = entering_kv.shape

    partner_kv = other_core(every_second_head(entering_kv, (1 - core)[None]))
    partner_weights = [other_core(w) for w in (w_query, w_out, w_gate, w_up, w_down)]
    order = token_order(tokens, chip, core)
    entered = tokens // 2
    groups = max(1, entered // 128)
    each = requests // groups
    mask_shape = (groups, 2 * each * positions, entered // groups)
    row = lax.broadcasted_iota(jnp.int32, mask_shape, 1)
    source = jnp.where(row // (each * positions) == 0, core, 1 - core)
    at = (2 * chip + source) * positions + row % positions
    lengths = jnp.broadcast_to(
        enc_lengths[0].reshape(groups, 1, each, 1), (groups, 2, each, positions)
    ).reshape(mask_shape[:2])
    same = (row // positions) % each == lax.broadcasted_iota(jnp.int32, mask_shape, 2) // QLEN
    usable = (same & (at < lengths[:, :, None])).astype(jnp.float32)
    heads = (chip + jnp.array(SLOTS, jnp.int32)) % RING
    columns = jnp.stack([2 * heads + core, heads])

    def query_of(w, x):
        return lax.dot_general(
            w, x, (((0,), (1,)), ((), ())), preferred_element_type=jnp.float32
        ).astype(jnp.bfloat16)

    normed, (partner_kv, partner_weights, order, usable, columns) = ring_gather(
        normalize(hidden, norm_gain_attn), (partner_kv, partner_weights, order, usable, columns)
    )
    normed = normed.reshape(mine, width)
    query_p, out_p, gate_p, up_p, down_p = partner_weights
    arrived = other_core(query_of(query_p, normed))
    query = jnp.concatenate([query_of(w_query, normed), arrived], axis=1)
    query = jnp.dot(query, order, preferred_element_type=jnp.float32).astype(jnp.bfloat16)

    gathered_query, _ = ring_gather(query[:, :entered])
    parts = partial_attention(gathered_query, entering_kv, partner_kv, usable, columns)
    context_entering = close_parts(*ring_reduce(parts, join_parts, join_parts, lambda x: x))
    context_cached = attend(query[:, entered:].T, cached_kv, enc_lengths[1]).T
    context = jnp.concatenate([context_entering, context_cached], axis=1)
    context = lax.dot_general(
        context, order, (((1,), (1,)), ((), ())), preferred_element_type=jnp.float32
    ).astype(jnp.bfloat16)

    def out_product(x, w):
        return lax.dot_general(x, w, (((0,), (0,)), ((), ())), preferred_element_type=jnp.float32)

    arrived = other_core(context[:, mine:])
    product = out_product(context[:, :mine], w_out) + out_product(arrived, out_p)
    attention = sum_over_ring(product.reshape(RING, rows, width))
    residual = (hidden.astype(jnp.float32) + attention).astype(jnp.bfloat16)

    def feed(x, gate_w, up_w, down_w):
        gate = jnp.dot(x, gate_w, preferred_element_type=jnp.float32)
        upward = jnp.dot(x, up_w, preferred_element_type=jnp.float32)
        activated = (jax.nn.gelu(gate, approximate=True) * upward).astype(jnp.bfloat16)
        return jnp.dot(activated, down_w, preferred_element_type=jnp.float32)

    normed, _ = ring_gather(normalize(residual, norm_gain_ffn))
    normed = normed.reshape(mine, width)
    product = feed(normed, w_gate, w_up, w_down) + feed(normed, gate_p, up_p, down_p)
    feed_out = sum_over_ring(product.reshape(RING, rows, width))
    return (residual.astype(jnp.float32) + feed_out).astype(jnp.bfloat16)


def solution(mesh):
    torus = Mesh(mesh.devices.reshape(mesh.shape["groups"], RING, 2), ("groups", "mp_0", "mp_1"))
    in_specs = (
        P(GROUPS_MP, None),
        P(),
        P(None, MP),
        P("groups", MP, None),
        P("groups", None, MP),
        P(None, "groups"),
        P(MP, None),
        P(),
        P(None, MP),
        P(None, MP),
        P(MP, None),
    )
    out_specs = P(GROUPS_MP, None)
    return jax.shard_map(
        per_device, mesh=torus, in_specs=in_specs, out_specs=out_specs, check_vma=False
    )
```
